32 devices in a mesh: gx: 8 (over z, x), gy: 4 (over y, core).
Axes of the slice: x: 2, y: 2, z: 4, core: 2. Of those that a mesh axis runs over, the one named last changes fastest.
Arguments:
- velocity: float32 [2, 1024, 1024], P(None, 'gy', 'gx'), may hold values from -3 to 3
- stress: float32 [3, 1024, 1024], P(None, 'gy', 'gx'), may hold values from -3 to 3
- ice_mass: float32 [1024, 1024], P('gy', 'gx'), may hold values from 0.5 to 4
- strength: float32 [1024, 1024], P('gy', 'gx'), may hold values from 0.2 to 2
- land_mask: int32 [1024, 1024], P('gy', 'gx'), may hold values from 0 to 1
- ocean_forcing: float32 [4, 1024, 1024], P(None, ('gy', 'gx')), may hold values from -3 to 3
Outputs:
- velocity_out: float32 [2, 1024, 1024], P(None, 'gy', 'gx')
- stress_out: float32 [3, 1024, 1024], P(None, 'gy', 'gx')
- residuals: float32 [4], replicated
- ocean_stress: float32 [2, 1024, 1024], P(None, ('gy', 'gx'))
The draws below stay inside these ranges and needn't reach their ends.
All inputs are finite; a program needn't handle non-finite values.
Results may differ from the reference program's by a relative error of at most 0.0001.
Values sent between devices are 32-bit elements; how exact they have to be, the bound alone decides.
No kernel may reach another device: no remote copies, remote signals or barrier semaphores. Data moves between devices by JAX's collectives and lax.ppermute only.
A program may use at most 64 MiB of HBM per device.

```python
import math
import jax
import jax.numpy as jnp
from jax import lax

ITERS = 4
NX = 1024
NY = 1024


def draw_land_mask(key, part):
    lon_index = lax.broadcasted_iota(jnp.int32, (NY, NX), 1)
    lat_index = lax.broadcasted_iota(jnp.int32, (NY, NX), 0)
    threshold = 100 + 300 * lon_index // NX + 300 * lat_index // NY
    rolled = jax.random.randint(jax.random.fold_in(key, 17), (NY, NX), 0, 1000)
    return (rolled >= threshold).astype(jnp.int32)


def levels(stream_key, shape, pieces, low, largest):
    def one(axis_at, blocks):
        steps = jax.random.uniform(jax.random.fold_in(jax.random.fold_in(stream_key, 6), axis_at), (blocks,), jnp.float32, low / len(pieces), largest / len(pieces))
        return jnp.repeat(jnp.exp(steps), shape[axis_at] // blocks).reshape((-1,) + (1,) * (len(shape) - axis_at - 1))

    gain = one(*pieces[0])
    for cut in pieces[1:]:
        gain = gain * one(*cut)
    return gain


def normal_values(key, shape, deviation, bound, cuts=(), dtype=jnp.bfloat16):
    level = levels(key, shape, cuts, -0.22, 0.18) if cuts else 1.0
    values = jax.random.normal(key, shape, jnp.float32) * deviation * level
    return jnp.minimum(jnp.maximum(values, -bound), bound).astype(dtype)


def setup_inputs(seed: int = 0) -> dict:
    key_list = jax.random.split(jax.random.key(seed), 7)
    return {
        "velocity": normal_values(key_list[0], (2, NY, NX), 0.5, 3.0, ((1, 4), (2, 8)), jnp.float32),
        "stress": normal_values(key_list[1], (3, NY, NX), 0.5, 3.0, ((1, 4), (2, 8)), jnp.float32),
        "ice_mass": jnp.clip(jnp.exp(math.log(4.0) - 2.0794415 * jax.random.uniform(key_list[2], (NY, NX), jnp.float32) ** levels(key_list[2], (NY, NX), ((0, 4), (1, 8)), -0.2, 0.2)), 0.5, 4.0),
        "strength": jnp.clip(jnp.exp(math.log(2.0) - 2.3025851 * jax.random.uniform(key_list[3], (NY, NX), jnp.float32) ** levels(key_list[3], (NY, NX), ((0, 4), (1, 8)), -0.2, 0.2)), 0.2, 2.0),
        "land_mask": draw_land_mask(jax.random.fold_in(key_list[6], 71), 0),
        "ocean_forcing": normal_values(key_list[5], (4, NY, NX), 0.5, 3.0, ((1, 32),), jnp.float32),
    }


ALPHA = 4.0
BETA = 4.0
WATER_DRAG = 1.0
DELTA_FLOOR = 0.0025

def extend_field(field):
    wrapped = jnp.concatenate([field[..., -1:], field, field[..., :1]], axis=-1)
    padding = [(0, 0)] * (field.ndim - 2) + [(1, 1), (0, 0)]
    return jnp.pad(wrapped, padding)

def diff_east(padded):
    return 0.5 * (padded[..., 1:-1, 2:] - padded[..., 1:-1, :-2])

def diff_north(padded):
    return 0.5 * (padded[..., 2:, 1:-1] - padded[..., :-2, 1:-1])

def relax_stress(padded_vel, stress, strength, ice_frac):
    east_dx = diff_east(padded_vel[0])
    east_dy = diff_north(padded_vel[0])
    north_dx = diff_east(padded_vel[1])
    north_dy = diff_north(padded_vel[1])
    divergence = east_dx + north_dy
    tension = east_dx - north_dy
    shear_rate = east_dy + north_dx
    delta_rate = jnp.sqrt(divergence * divergence + 0.25 * (tension * tension + shear_rate * shear_rate) + DELTA_FLOOR)
    target = jnp.stack([strength * (divergence / delta_rate - 1.0), strength * tension / (4.0 * delta_rate), strength * shear_rate / (8.0 * delta_rate)])
    return (stress + (target - stress) / ALPHA) * ice_frac

def drag_coeff(vel, currents):
    east_gap = currents[0] - vel[0]
    north_gap = currents[1] - vel[1]
    return WATER_DRAG * jnp.sqrt(east_gap * east_gap + north_gap * north_gap + 0.01)

def relax_velocity(padded_stress, vel, vel_start, forcing, ice_mass, coriolis, ice_frac):
    normal_xx = 0.5 * (padded_stress[0] + padded_stress[1])
    normal_yy = 0.5 * (padded_stress[0] - padded_stress[1])
    shear_xy = padded_stress[2]
    force_east = diff_east(normal_xx) + diff_north(shear_xy)
    force_north = diff_east(shear_xy) + diff_north(normal_yy)
    drag_rate = drag_coeff(vel, forcing[2:4])
    denominator = BETA + 1.0 + drag_rate / ice_mass
    new_east = (BETA * vel[0] + vel_start[0] + (force_east + forcing[0] + drag_rate * forcing[2]) / ice_mass + coriolis * vel[1]) / denominator * ice_frac
    new_north = (BETA * vel[1] + vel_start[1] + (force_north + forcing[1] + drag_rate * forcing[3]) / ice_mass - coriolis * vel[0]) / denominator * ice_frac
    return jnp.stack([new_east, new_north])

def reference(velocity, stress, ice_mass, strength, land_mask, ocean_forcing):
    ice_frac = land_mask.astype(jnp.float32)
    lat_rows = jnp.arange(NY).astype(jnp.float32)
    coriolis = (0.3 + 1.2 * (lat_rows + 0.5) / NY)[:, None]
    vel = velocity
    history = []
    for subcycle in range(ITERS):
        stress = relax_stress(extend_field(vel), stress, strength, ice_frac)
        new_vel = relax_velocity(extend_field(stress), vel, velocity, ocean_forcing, ice_mass, coriolis, ice_frac)
        change = new_vel - vel
        history.append(jnp.sum(change * change))
        vel = new_vel
    drag_rate = drag_coeff(vel, ocean_forcing[2:4])
    ocean_stress = drag_rate * (vel - ocean_forcing[2:4]) * ice_frac
    return (vel, stress, jnp.stack(history), ocean_stress)
```

```python
import functools

import jax
import jax.numpy as jnp
from jax import lax
from jax.experimental import pallas as pl
from jax.experimental.pallas import tpu as pltpu
from jax.sharding import PartitionSpec as P


ITERS = 4
DELTA_FLOOR = 0.0025
DEPTH = 2 * ITERS
SLOT = 2 * DEPTH
FIELDS = 8
PAD = 2 * DEPTH

SMEM = pl.BlockSpec(memory_space=pltpu.SMEM)
VMEM = pl.BlockSpec(memory_space=pltpu.VMEM)
F32 = jnp.float32


def call(body, name, n_in, outs, scratch=(), scalars=1):
    return pl.pallas_call(
        body,
        out_shape=[jax.ShapeDtypeStruct(s, F32) for s in outs],
        in_specs=[SMEM] * scalars + [VMEM] * n_in,
        out_specs=[VMEM] * len(outs),
        scratch_shapes=[pltpu.VMEM(s, F32) for s in scratch],
        name=name,
    )


def lane_of(shape):
    return lax.broadcasted_iota(jnp.int32, shape, 1)


def slot_start(index):
    return SLOT * index


def transposed(tile, lanes):
    rows = tile.shape[0]
    if rows < lanes:
        tile = jnp.concatenate([tile, jnp.zeros((lanes - rows, lanes), F32)], axis=0)
    parts = [tile[i : i + lanes].T for i in range(0, tile.shape[0], lanes)]
    return parts[0] if len(parts) == 1 else jnp.concatenate(parts, axis=1)


def pack_fields(scal, vel, sig, strength, mass, mask, to_right, to_left):
    cols = vel.shape[2]
    planes = [vel[0], vel[1], sig[0], sig[1], sig[2], strength[...], mass[...], mask[...].astype(F32)]
    lane = lane_of(planes[0].shape)
    tile = jnp.zeros(planes[0].shape, F32)
    for i, plane in enumerate(planes):
        start = slot_start(i)
        moved = pltpu.roll(plane, (DEPTH + start) % cols, 1)
        tile = jnp.where((lane >= start) & (lane < start + SLOT), moved, tile)
    turned = transposed(tile, cols)
    for i in range(FIELDS):
        start = slot_start(i)
        to_right[i * DEPTH : (i + 1) * DEPTH, :] = turned[start : start + DEPTH]
        to_left[i * DEPTH : (i + 1) * DEPTH, :] = turned[start + DEPTH : start + SLOT]


def pack_forcing(xor, n, scal, band, *refs):
    outs, turned_ref = refs[:-1], refs[-1]
    kinds, rows, width = band.shape
    cols = width // n
    height = kinds * rows
    me = scal[0]
    lane = lane_of((height, cols))
    per_tile = cols // SLOT
    tiles = [band[:, :, d * cols : (d + 1) * cols].reshape(height, cols) for d in range(n)]
    for first in range(0, n, per_tile):
        packed = jnp.zeros((height, cols), F32)
        for d in range(first, min(first + per_tile, n)):
            start = slot_start(d - first)
            halo = jnp.where(lane < cols // 2, tiles[(d + 1) % n], tiles[(d - 1) % n])
            moved = pltpu.roll(halo, (DEPTH + start) % cols, 1)
            packed = jnp.where((lane >= start) & (lane < start + SLOT), moved, packed)
        turned_ref[first * SLOT : first * SLOT + cols, :] = transposed(packed, cols)
    for k in range(n):
        d = me ^ k if xor else k
        out = outs[k] if xor else outs[0].at[k]
        at = pl.multiple_of(d * cols, cols) if xor else d * cols
        out[:height, :] = band[:, :, pl.ds(at, cols)].reshape(height, cols)
        at = pl.multiple_of(d * SLOT, SLOT) if xor else d * SLOT
        out[height:, :] = turned_ref[pl.ds(at, SLOT), :]


def extend_fields(scal, vel, sig, strength, mass, mask, from_left, from_right, ext, to_up, to_down):
    rows, cols = strength.shape
    planes = [vel[0], vel[1], sig[0], sig[1], sig[2], strength[...], mass[...], mask[...].astype(F32)]
    pieces = []
    for i in range(FIELDS):
        pieces.append(from_left[i * DEPTH : (i + 1) * DEPTH, :])
        pieces.append(from_right[i * DEPTH : (i + 1) * DEPTH, :])
    turned = jnp.concatenate(pieces, axis=0)
    halo = jnp.concatenate([turned[:, i : i + cols].T for i in range(0, rows, cols)], axis=0)
    for i, plane in enumerate(planes):
        wing = pltpu.roll(halo, (-(DEPTH + slot_start(i))) % cols, 1)
        for out, lo, hi in ((ext.at[i], PAD, PAD + rows),):
            out[lo:hi, :cols] = plane
            out[lo:hi, cols:] = wing
        to_up[i * DEPTH : (i + 1) * DEPTH, :cols] = plane[:DEPTH]
        to_up[i * DEPTH : (i + 1) * DEPTH, cols:] = wing[:DEPTH]
        to_down[i * DEPTH : (i + 1) * DEPTH, :cols] = plane[rows - DEPTH :]
        to_down[i * DEPTH : (i + 1) * DEPTH, cols:] = wing[rows - DEPTH :]


def shifts(ref, base, height):
    around = ref.at[pl.ds(base - DEPTH, height + 2 * DEPTH), :]
    return tuple(around[DEPTH + step : DEPTH + step + height, :] for step in (0, -1, 1))


def east_west(x):
    width = x.shape[1]
    return pltpu.roll(x, width - 1, 1) - pltpu.roll(x, 1, 1)


def stress_block(u_ref, v_ref, base, height, old_a, old_b, old_w, p4, ice):
    u, u_m, u_p = shifts(u_ref, base, height)
    v, v_m, v_p = shifts(v_ref, base, height)
    ux, uy = east_west(u), u_p - u_m
    vx, vy = east_west(v), v_p - v_m
    div = 0.5 * (ux + vy)
    ten = 0.125 * (ux - vy)
    shear = 0.125 * (uy + vx)
    inv = lax.rsqrt(div * div + 4.0 * (ten * ten + shear * shear) + DELTA_FLOOR)
    pr = p4 * inv
    keep = 0.75 * ice
    return (
        keep * old_a + (pr * (div + ten) - p4),
        keep * old_b + (pr * (div - ten) - p4),
        keep * old_w + pr * shear,
    )


def first_stress(scal, ext, top, bottom, vel_a, state, fixed):
    total = scal[2]
    row_start = scal[1]
    rows = ext.shape[1] - 2 * PAD
    width = ext.shape[2]
    for i in range(FIELDS):
        ext_i = ext.at[i]
        for at, src, alive in ((DEPTH, top, row_start > 0), (PAD + rows, bottom, row_start + rows < total)):
            piece = src[i * DEPTH : (i + 1) * DEPTH, :]
            if i < 2:
                vel_a[i, at : at + DEPTH, :] = jnp.where(alive, piece, 0.0)
            elif i == 7:
                fixed[1, at : at + DEPTH, :] = jnp.where(alive, piece, 0.0)
    height = 2 * DEPTH

    def copy(base, src, off):
        return src[off : off + DEPTH, :]

    def setup(base, count, get, alive):
        keep = (lambda x: x) if alive is None else (lambda x: jnp.where(alive, x, 0.0))
        ice = keep(get(7))
        vel_a[0, pl.ds(base, count), :] = keep(get(0))
        vel_a[1, pl.ds(base, count), :] = keep(get(1))
        s0, s1 = get(2), get(3)
        state[0, pl.ds(base, count), :] = s0 + s1
        state[1, pl.ds(base, count), :] = s0 - s1
        state[2, pl.ds(base, count), :] = 2.0 * get(4)
        fixed[0, pl.ds(base, count), :] = 0.25 * get(5) * ice
        fixed[1, pl.ds(base, count), :] = ice
        fixed[2, pl.ds(base, count), :] = 1.0 / get(6)

    setup(DEPTH, DEPTH, lambda i: top[i * DEPTH : (i + 1) * DEPTH, :], row_start > 0)
    setup(PAD + rows, DEPTH, lambda i: bottom[i * DEPTH : (i + 1) * DEPTH, :], row_start + rows < total)

    def own(t, carry):
        base = pl.multiple_of(PAD + t * height, DEPTH)
        setup(base, height, lambda i: ext[i, pl.ds(base, height), :], None)
        return carry

    lax.fori_loop(0, rows // height, own, 0)

    def step(t, carry):
        base = pl.multiple_of(DEPTH + t * height, DEPTH)
        at = pl.ds(base, height)
        a, b, w = stress_block(
            vel_a.at[0], vel_a.at[1], base, height, state[0, at, :], state[1, at, :], state[2, at, :], fixed[0, at, :], fixed[1, at, :]
        )
        state[0, at, :] = a
        state[1, at, :] = b
        state[2, at, :] = w
        return carry

    lax.fori_loop(0, (rows + 2 * DEPTH) // height, step, 0)


def extend_forcing(xor, n, scal, *refs):
    count = n if xor else 1
    blocks, (ext, to_up, to_down) = refs[:count], refs[count : count + 3]
    turned_ref = refs[count + 3]
    me = scal[0]
    kinds = ext.shape[0]
    cols = ext.shape[2] // 2
    rows = ext.shape[1] - 2 * PAD
    band = rows // n
    height = kinds * band
    per_tile = cols // SLOT
    for k in range(n):
        block = blocks[k] if xor else blocks[0].at[k]
        source = me ^ k if xor else k
        base = pl.multiple_of(PAD + source * band, DEPTH) if xor else PAD + source * band
        for f in range(kinds):
            ext[f, pl.ds(base, band), :cols] = block[f * band : (f + 1) * band, :]
        turned_ref[k * SLOT : (k + 1) * SLOT, :] = block[height : height + SLOT, :]
    for first in range(0, n, per_tile):
        span = min(per_tile, n - first) * SLOT
        piece = turned_ref[first * SLOT : first * SLOT + span, :]
        if span < cols:
            piece = jnp.concatenate([piece, jnp.zeros((cols - span, cols), F32)], axis=0)
        halo = piece.T
        for k in range(first, min(first + per_tile, n)):
            source = me ^ k if xor else k
            base = pl.multiple_of(PAD + source * band, DEPTH) if xor else PAD + source * band
            wing = pltpu.roll(halo, (-(DEPTH + slot_start(k - first))) % cols, 1)
            for f in range(kinds):
                ext[f, pl.ds(base, band), cols:] = wing[f * band : (f + 1) * band]
    for f in range(kinds):
        to_up[f * DEPTH : (f + 1) * DEPTH, :] = ext[f, PAD : PAD + DEPTH, :]
        to_down[f * DEPTH : (f + 1) * DEPTH, :] = ext[f, PAD + rows - DEPTH : PAD + rows, :]


def velocity_block(u, v, state, base, height, im, ice, be, bn, oe, on, cor):
    a = state[0, pl.ds(base, height), :]
    w, w_m, w_p = shifts(state.at[2], base, height)
    _, b_m, b_p = shifts(state.at[1], base, height)
    if u.shape[1] < a.shape[1]:
        cut = u.shape[1]
        ge = east_west(a)[:, :cut] + (w_p[:, :cut] - w_m[:, :cut])
        gn = east_west(w)[:, :cut] + (b_p[:, :cut] - b_m[:, :cut])
    else:
        ge = east_west(a) + (w_p - w_m)
        gn = east_west(w) + (b_p - b_m)
    gap_e, gap_n = oe - u, on - v
    square = gap_e * gap_e + gap_n * gap_n + 0.01
    pull = square * lax.rsqrt(square) * im
    inv = ice / (pull + 5.0)
    im4 = 0.25 * im
    new_u = (4.0 * u + be + ge * im4 + pull * oe + cor * v) * inv
    new_v = (4.0 * v + bn + gn * im4 + pull * on - cor * u) * inv
    return new_u, new_v


def subcycles(xor, n, scal, vel0, state0, fixed, forcing, top, bottom, vel_out, sig_out, *refs):
    blocks, (vel, state, base_ref, ocean) = refs[:-4], refs[-4:]
    me, row_start, total = scal[0], scal[1], scal[2]
    rows = vel0.shape[1] - 2 * PAD
    cols = vel_out.shape[2]
    height = 2 * DEPTH
    band = rows // n
    scale = 1.2 / total.astype(F32)

    def coriolis(base, count, width):
        row = lax.broadcasted_iota(jnp.int32, (count, width), 0) + (row_start + base - PAD)
        return 0.3 + scale * (row.astype(F32) + 0.5)

    def put_forcing(base, count, get):
        at = pl.ds(base, count)
        im = fixed[2, at, :]
        base_ref[0, at, :] = vel0[0, at, :] + get(0) * im
        base_ref[1, at, :] = vel0[1, at, :] + get(1) * im
        ocean[0, at, :] = get(2)
        ocean[1, at, :] = get(3)

    put_forcing(DEPTH, DEPTH, lambda f: top[f * DEPTH : (f + 1) * DEPTH, :])
    put_forcing(PAD + rows, DEPTH, lambda f: bottom[f * DEPTH : (f + 1) * DEPTH, :])

    def own(t, carry):
        base = pl.multiple_of(PAD + t * height, DEPTH)
        put_forcing(base, height, lambda f: forcing[f, pl.ds(base, height), :])
        return carry

    lax.fori_loop(0, rows // height, own, 0)

    def stress_sweep(old):
        def step(t, carry):
            base = pl.multiple_of(DEPTH + t * height, DEPTH)
            at = pl.ds(base, height)
            a, b, w = stress_block(
                vel.at[0], vel.at[1], base, height, old[0, at, :], old[1, at, :], old[2, at, :], fixed[0, at, :], fixed[1, at, :]
            )
            state[0, at, :] = a
            state[1, at, :] = b
            state[2, at, :] = w
            return carry

        lax.fori_loop(0, (rows + 2 * DEPTH) // height, step, 0)

    def velocity_sweep(old_vel, now):
        def step(t, acc):
            base = pl.multiple_of(DEPTH + t * height, DEPTH)
            at = pl.ds(base, height)
            u, v = old_vel[0, at, :], old_vel[1, at, :]
            new_u, new_v = velocity_block(
                u, v, now, base, height, fixed[2, at, :], fixed[1, at, :], base_ref[0, at, :], base_ref[1, at, :],
                ocean[0, at, :], ocean[1, at, :], coriolis(base, height, 2 * cols),
            )
            vel[0, at, :] = new_u
            vel[1, at, :] = new_v
            du, dv = (new_u - u)[:, :cols], (new_v - v)[:, :cols]
            gain = du * du + dv * dv
            row = lax.broadcasted_iota(jnp.int32, gain.shape, 0) + base
            return acc + jnp.where((row >= PAD) & (row < PAD + rows), gain, 0.0)

        return lax.fori_loop(0, (rows + 2 * DEPTH) // height, step, jnp.zeros((height, cols), F32))

    sums = []
    for cycle in range(ITERS - 1):
        if cycle:
            stress_sweep(state0 if cycle == 1 else state)
        sums.append(velocity_sweep(vel0 if cycle == 0 else vel, state0 if cycle == 0 else state))
    stress_sweep(state)

    def last(d, acc):
        base = pl.multiple_of(PAD + d * band, DEPTH)
        at = pl.ds(base, band)
        u, v = vel[0, at, :cols], vel[1, at, :cols]
        oe, on = ocean[0, at, :cols], ocean[1, at, :cols]
        ice = fixed[1, at, :cols]
        new_u, new_v = velocity_block(
            u, v, state, base, band, fixed[2, at, :cols], ice, base_ref[0, at, :cols], base_ref[1, at, :cols],
            oe, on, coriolis(base, band, cols),
        )
        a, b, w = state[0, at, :cols], state[1, at, :cols], state[2, at, :cols]
        to = pl.ds(pl.multiple_of(d * band, DEPTH), band)
        vel_out[0, to, :] = new_u
        vel_out[1, to, :] = new_v
        sig_out[0, to, :] = 0.5 * (a + b)
        sig_out[1, to, :] = 0.5 * (a - b)
        sig_out[2, to, :] = 0.5 * w
        gap_e, gap_n = new_u - oe, new_v - on
        square = gap_e * gap_e + gap_n * gap_n + 0.01
        drag = square * lax.rsqrt(square) * ice
        blocks[0][d, :band, :] = drag * gap_e
        blocks[0][d, band : 2 * band, :] = drag * gap_n
        du, dv = new_u - u, new_v - v
        return acc + (du * du + dv * dv)

    sums.append(lax.fori_loop(0, n, last, jnp.zeros((band, cols), F32)))
    lines = [jnp.sum(s, axis=0, keepdims=True) for s in sums]
    tail = jnp.concatenate(lines + [jnp.zeros((DEPTH - ITERS, cols), F32)], axis=0)
    for k in range(n):
        blocks[0][k, 2 * band :, :] = tail


def unpack_out(n, got, out, sums):
    band, width = out.shape[1], out.shape[2]
    cols = width // n
    for k in range(n):
        for f in range(2):
            out[f, :, k * cols : (k + 1) * cols] = got[k, f * band : (f + 1) * band, :]
    total = got[0, 2 * band :, :]
    for k in range(1, n):
        total = total + got[k, 2 * band :, :]
    sums[...] = total


def total_sums(*refs):
    total = refs[0][...]
    for r in refs[1:-1]:
        total = total + r[...]
    refs[-1][...] = jnp.broadcast_to(jnp.sum(total, axis=1, keepdims=True), total.shape)


def local(velocity, stress, ice_mass, strength, land_mask, ocean_forcing):
    rows, cols = velocity.shape[1], velocity.shape[2]
    n, m = lax.axis_size("gx"), lax.axis_size("gy")
    band = ocean_forcing.shape[1]
    kinds = ocean_forcing.shape[0]
    xor = n & (n - 1) == 0 and n <= 8
    tall = rows + 2 * PAD
    me = lax.axis_index("gx")
    scal = jnp.stack([me, lax.axis_index("gy") * rows, m * rows]).astype(jnp.int32)

    def shift(x, axis, step):
        count = lax.axis_size(axis)
        return lax.ppermute(x, axis, [(i, (i + step) % count) for i in range(count)])

    def swap(x, axis, k):
        return lax.ppermute(x, axis, [(i, i ^ k) for i in range(lax.axis_size(axis))])

    fields = (velocity, stress, strength, ice_mass, land_mask)
    to_right, to_left = call(pack_fields, "pack_fields", 5, [(FIELDS * DEPTH, rows)] * 2)(scal, *fields)
    block = (kinds * band + SLOT, cols)
    slots = -(-n * SLOT // cols) * cols
    packed = call(
        functools.partial(pack_forcing, xor, n), "pack_forcing", 1, [block] * n if xor else [(n,) + block],
        scratch=[(slots, cols)],
    )(scal, ocean_forcing)
    from_left = shift(to_right, "gx", 1)
    from_right = shift(to_left, "gx", -1)
    if xor:
        got = [packed[0]] + [None] * (n - 1)
        for k in range(n - 1, 0, -1):
            got[k] = swap(packed[k], "gx", k)
    else:
        got = [lax.all_to_all(packed[0], "gx", split_axis=0, concat_axis=0, tiled=True)]

    ext, to_up, to_down = call(
        extend_fields, "extend_fields", 7,
        [(FIELDS, tall, 2 * cols), (FIELDS * DEPTH, 2 * cols), (FIELDS * DEPTH, 2 * cols)],
    )(scal, *fields, from_left, from_right)
    bottom = shift(to_up, "gy", -1)
    top = shift(to_down, "gy", 1)
    vel0, state0, fixed = call(
        first_stress, "first_stress", 3, [(2, tall, 2 * cols), (3, tall, 2 * cols), (3, tall, 2 * cols)]
    )(scal, ext, top, bottom)

    forcing, f_up, f_down = call(
        functools.partial(extend_forcing, xor, n), "extend_forcing", len(got),
        [(kinds, tall, 2 * cols), (kinds * DEPTH, 2 * cols), (kinds * DEPTH, 2 * cols)],
        scratch=[(slots, cols)],
    )(scal, *got)
    f_bottom = shift(f_up, "gy", -1)
    f_top = shift(f_down, "gy", 1)
    vel, sig, blocks = call(
        functools.partial(subcycles, xor, n), "subcycles", 6,
        [velocity.shape, stress.shape, (n, 2 * band + DEPTH, cols)],
        scratch=[(2, tall, 2 * cols), (3, tall, 2 * cols), (2, tall, 2 * cols), (2, tall, 2 * cols)],
    )(scal, vel0, state0, fixed, forcing, f_top, f_bottom)
    back = lax.all_to_all(blocks, "gx", split_axis=0, concat_axis=0, tiled=True)
    ocean_stress, sums = call(
        functools.partial(unpack_out, n), "unpack_out", 1, [(2, band, n * cols), (DEPTH, cols)], scalars=0
    )(back)
    others = [sums] + [shift(sums, "gy", k) for k in range(1, m)]
    (history,) = call(total_sums, "total_sums", m, [(DEPTH, cols)], scalars=0)(*others)
    return vel, sig, history[:ITERS, 0], ocean_stress


def solution(mesh):
    placed = (
        P(None, "gy", "gx"),
        P(None, "gy", "gx"),
        P("gy", "gx"),
        P("gy", "gx"),
        P("gy", "gx"),
        P(None, ("gy", "gx"), None),
    )
    return jax.shard_map(
        local,
        mesh=mesh,
        in_specs=placed,
        out_specs=(P(None, "gy", "gx"), P(None, "gy", "gx"), P(), P(None, ("gy", "gx"), None)),
        check_vma=False,
    )
```

```python
import functools

import jax
import jax.numpy as jnp
from jax import lax
from jax.experimental import pallas as pl
from jax.experimental.pallas import tpu as pltpu
from jax.sharding import PartitionSpec as P


ITERS = 4
DELTA_FLOOR = 0.0025
DEPTH = 2 * ITERS
SLOT = 2 * DEPTH
FIELDS = 8
PAD = 2 * DEPTH

SMEM = pl.BlockSpec(memory_space=pltpu.SMEM)
VMEM = pl.BlockSpec(memory_space=pltpu.VMEM)
F32 = jnp.float32
VMEM_LIMIT = 16 * 1024 * 1024


def call(body, name, n_in, outs, scratch=(), scalars=1, space=None):
    return pl.pallas_call(
        body,
        out_shape=[jax.ShapeDtypeStruct(s, F32) for s in outs],
        in_specs=[SMEM] * scalars + [space or VMEM] * n_in,
        out_specs=[VMEM] * len(outs),
        scratch_shapes=scratch,
        name=name,
        compiler_params=pltpu.CompilerParams(vmem_limit_bytes=VMEM_LIMIT),
    )


def planes_of(*shapes):
    return [pltpu.VMEM(s, F32) for s in shapes]


def lane_of(shape):
    return lax.broadcasted_iota(jnp.int32, shape, 1)


def slot_start(index):
    return SLOT * index


def transposed(tile, lanes):
    rows = tile.shape[0]
    if rows < lanes:
        tile = jnp.concatenate([tile, jnp.zeros((lanes - rows, lanes), F32)], axis=0)
    parts = [tile[i : i + lanes].T for i in range(0, tile.shape[0], lanes)]
    return parts[0] if len(parts) == 1 else jnp.concatenate(parts, axis=1)


def pack(xor, n, scal, vel, sig, strength, mass, mask, band_hbm, own, to_right, to_left, *refs):
    outs, (mask_ref, band, turned_ref, sems) = refs[:-4], refs[-4:]
    copies = [
        pltpu.make_async_copy(src, dst, sems.at[i])
        for i, (src, dst) in enumerate(
            (
                (vel, own.at[0:2]),
                (sig, own.at[2:5]),
                (strength, own.at[5]),
                (mass, own.at[6]),
                (mask, mask_ref),
                (band_hbm, band),
            )
        )
    ]
    for c in copies:
        c.start()
    for c in copies[:-1]:
        c.wait()
    own[7] = mask_ref[...].astype(F32)
    cols = own.shape[2]
    lane = lane_of(own.shape[1:])
    tile = jnp.zeros(own.shape[1:], F32)
    for i in range(FIELDS):
        start = slot_start(i)
        moved = pltpu.roll(own[i], (DEPTH + start) % cols, 1)
        tile = jnp.where((lane >= start) & (lane < start + SLOT), moved, tile)
    turned = transposed(tile, cols)
    for i in range(FIELDS):
        start = slot_start(i)
        to_right[i * DEPTH : (i + 1) * DEPTH, :] = turned[start : start + DEPTH]
        to_left[i * DEPTH : (i + 1) * DEPTH, :] = turned[start + DEPTH : start + SLOT]

    kinds, rows, _ = band.shape
    height = kinds * rows
    me = scal[0]
    lane = lane_of((height, cols))
    per_tile = cols // SLOT
    copies[-1].wait()
    tiles = [band[:, :, d * cols : (d + 1) * cols].reshape(height, cols) for d in range(n)]
    for first in range(0, n, per_tile):
        packed = jnp.zeros((height, cols), F32)
        for d in range(first, min(first + per_tile, n)):
            start = slot_start(d - first)
            halo = jnp.where(lane < cols // 2, tiles[(d + 1) % n], tiles[(d - 1) % n])
            moved = pltpu.roll(halo, (DEPTH + start) % cols, 1)
            packed = jnp.where((lane >= start) & (lane < start + SLOT), moved, packed)
        turned_ref[first * SLOT : first * SLOT + cols, :] = transposed(packed, cols)
    for k in range(n):
        d = me ^ k if xor else k
        out = outs[k] if xor else outs[0].at[k]
        at = pl.multiple_of(d * cols, cols) if xor else d * cols
        out[:height, :] = band[:, :, pl.ds(at, cols)].reshape(height, cols)
        at = pl.multiple_of(d * SLOT, SLOT) if xor else d * SLOT
        out[height:, :] = turned_ref[pl.ds(at, SLOT), :]


def extend_fields(scal, own, from_left, from_right, wings, to_up, to_down):
    _, rows, cols = own.shape
    pieces = []
    for i in range(FIELDS):
        pieces.append(from_left[i * DEPTH : (i + 1) * DEPTH, :])
        pieces.append(from_right[i * DEPTH : (i + 1) * DEPTH, :])
    turned = jnp.concatenate(pieces, axis=0)
    halo = jnp.concatenate([turned[:, i : i + cols].T for i in range(0, rows, cols)], axis=0)
    for i in range(FIELDS):
        wing = pltpu.roll(halo, (-(DEPTH + slot_start(i))) % cols, 1)
        wings[i] = wing
        to_up[i, 0] = own[i, :DEPTH, :]
        to_up[i, 1] = wing[:DEPTH]
        to_down[i, 0] = own[i, rows - DEPTH :, :]
        to_down[i, 1] = wing[rows - DEPTH :]


def shifted(ref, base, height, step):
    return ref.at[pl.ds(base - DEPTH, height + 2 * DEPTH), :][DEPTH + step : DEPTH + step + height, :]


def down_up(ref, at, base, height):
    return shifted(ref.at[at], base, height, 1) - shifted(ref.at[at], base, height, -1)


def east_west(main, wing):
    cols = main.shape[1]
    lane = lane_of(main.shape)
    east_m, east_w = pltpu.roll(main, cols - 1, 1), pltpu.roll(wing, cols - 1, 1)
    west_m, west_w = pltpu.roll(main, 1, 1), pltpu.roll(wing, 1, 1)
    end, begin = lane == cols - 1, lane == 0
    return (
        jnp.where(end, east_w, east_m) - jnp.where(begin, west_w, west_m),
        jnp.where(end, east_m, east_w) - jnp.where(begin, west_m, west_w),
    )


def east_west_of(ref, plane, base, height):
    at = pl.ds(base, height)
    return east_west(ref[plane, 0, at, :], ref[plane, 1, at, :])


def sweep(ref, planes, first, count, height, body, acc):
    for t in range(count):
        base = first + t * height
        acc = body(base, [east_west_of(ref, p, base, height) for p in planes], acc)
    return acc


def stress_sweep(vel, old, new, fixed, rows, height):
    def body(base, diffs, acc):
        at = pl.ds(base, height)
        for s in range(2):
            ux, vx = diffs[0][s], diffs[1][s]
            uy = down_up(vel, (0, s), base, height)
            vy = down_up(vel, (1, s), base, height)
            p4, ice = fixed[0, s, at, :], fixed[1, s, at, :]
            div = 0.5 * (ux + vy)
            ten = 0.125 * (ux - vy)
            shear = 0.125 * (uy + vx)
            inv = lax.rsqrt(div * div + 4.0 * (ten * ten + shear * shear) + DELTA_FLOOR)
            pr = p4 * inv
            keep = 0.75 * ice
            new[0, s, at, :] = keep * old[0, s, at, :] + (pr * (div + ten) - p4)
            new[1, s, at, :] = keep * old[1, s, at, :] + (pr * (div - ten) - p4)
            new[2, s, at, :] = keep * old[2, s, at, :] + pr * shear
        return acc

    sweep(vel, (0, 1), DEPTH, (rows + 2 * DEPTH) // height, height, body, 0)


def first_stress(scal, own, wings, top, bottom, vel, state, fixed):
    row_start, total = scal[1], scal[2]
    rows = own.shape[1]
    height = 2 * DEPTH

    def setup(base, count, s, get, alive):
        at = pl.ds(base, count)
        keep = (lambda x: x) if alive is None else (lambda x: jnp.where(alive, x, 0.0))
        ice = keep(get(7))
        vel[0, s, at, :] = keep(get(0))
        vel[1, s, at, :] = keep(get(1))
        s0, s1 = get(2), get(3)
        state[0, s, at, :] = s0 + s1
        state[1, s, at, :] = s0 - s1
        state[2, s, at, :] = 2.0 * get(4)
        fixed[0, s, at, :] = 0.25 * get(5) * ice
        fixed[1, s, at, :] = ice
        fixed[2, s, at, :] = 1.0 / get(6)

    for s in range(2):
        setup(DEPTH, DEPTH, s, lambda i: top[i, s], row_start > 0)
        setup(PAD + rows, DEPTH, s, lambda i: bottom[i, s], row_start + rows < total)

    for base in range(0, rows, height):
        for s, src in enumerate((own, wings)):
            setup(PAD + base, height, s, lambda i: src[i, pl.ds(base, height), :], None)
    stress_sweep(vel, state, state, fixed, rows, height)


def extend_forcing(xor, n, scal, *refs):
    count = n if xor else 1
    blocks, (ext, to_up, to_down) = refs[:count], refs[count : count + 3]
    turned_ref = refs[count + 3]
    me = scal[0]
    kinds, _, rows, cols = ext.shape
    band = rows // n
    height = kinds * band
    per_tile = cols // SLOT
    for k in range(n):
        block = blocks[k] if xor else blocks[0].at[k]
        source = me ^ k if xor else k
        base = pl.multiple_of(source * band, DEPTH) if xor else source * band
        for f in range(kinds):
            ext[f, 0, pl.ds(base, band), :] = block[f * band : (f + 1) * band, :]
        turned_ref[k * SLOT : (k + 1) * SLOT, :] = block[height : height + SLOT, :]
    for first in range(0, n, per_tile):
        span = min(per_tile, n - first) * SLOT
        piece = turned_ref[first * SLOT : first * SLOT + span, :]
        if span < cols:
            piece = jnp.concatenate([piece, jnp.zeros((cols - span, cols), F32)], axis=0)
        halo = piece.T
        for k in range(first, min(first + per_tile, n)):
            source = me ^ k if xor else k
            base = pl.multiple_of(source * band, DEPTH) if xor else source * band
            wing = pltpu.roll(halo, (-(DEPTH + slot_start(k - first))) % cols, 1)
            for f in range(kinds):
                ext[f, 1, pl.ds(base, band), :] = wing[f * band : (f + 1) * band]
    for f in range(kinds):
        for s in range(2):
            to_up[f, s] = ext[f, s, :DEPTH, :]
            to_down[f, s] = ext[f, s, rows - DEPTH :, :]


def subcycles(n, scal, vel0, state0, fixed, forcing, top, bottom, vel_out, sig_out, blocks, vel, state, start, ocean):
    row_start, total = scal[1], scal[2]
    rows, cols = vel_out.shape[1:]
    height = 2 * DEPTH
    band = rows // n
    scale = 1.2 / total.astype(F32)
    count = (rows + 2 * DEPTH) // height

    def coriolis(base, tall):
        row = lax.broadcasted_iota(jnp.int32, (tall, cols), 0) + (row_start + base - PAD)
        return 0.3 + scale * (row.astype(F32) + 0.5)

    def put_forcing(base, tall, s, get):
        at = pl.ds(base, tall)
        im = fixed[2, s, at, :]
        start[0, s, at, :] = vel0[0, s, at, :] + get(0) * im
        start[1, s, at, :] = vel0[1, s, at, :] + get(1) * im
        ocean[0, s, at, :] = get(2)
        ocean[1, s, at, :] = get(3)

    for s in range(2):
        put_forcing(DEPTH, DEPTH, s, lambda f: top[f, s])
        put_forcing(PAD + rows, DEPTH, s, lambda f: bottom[f, s])
    for base in range(0, rows, height):
        for s in range(2):
            put_forcing(PAD + base, height, s, lambda f: forcing[f, s, pl.ds(base, height), :])

    def moved(old, now, s, base, tall, diffs, cor):
        at = pl.ds(base, tall)
        ge = diffs[0][s] + down_up(now, (2, s), base, tall)
        gn = diffs[1][s] + down_up(now, (1, s), base, tall)
        u, v = old[0, s, at, :], old[1, s, at, :]
        oe, on = ocean[0, s, at, :], ocean[1, s, at, :]
        im, ice = fixed[2, s, at, :], fixed[1, s, at, :]
        gap_e, gap_n = oe - u, on - v
        square = gap_e * gap_e + gap_n * gap_n + 0.01
        pull = square * lax.rsqrt(square) * im
        inv = ice / (pull + 5.0)
        im4 = 0.25 * im
        new_u = (4.0 * u + start[0, s, at, :] + ge * im4 + pull * oe + cor * v) * inv
        new_v = (4.0 * v + start[1, s, at, :] + gn * im4 + pull * on - cor * u) * inv
        du, dv = new_u - u, new_v - v
        return new_u, new_v, du * du + dv * dv

    def velocity_sweep(old, now):
        def body(base, diffs, acc):
            at = pl.ds(base, height)
            cor = coriolis(base, height)
            for s in range(2):
                new_u, new_v, gain = moved(old, now, s, base, height, diffs, cor)
                vel[0, s, at, :] = new_u
                vel[1, s, at, :] = new_v
                if s == 0:
                    row = lax.broadcasted_iota(jnp.int32, gain.shape, 0) + base
                    acc = acc + jnp.where((row >= PAD) & (row < PAD + rows), gain, 0.0)
            return acc

        return sweep(now, (0, 2), DEPTH, count, height, body, jnp.zeros((height, cols), F32))

    sums = [velocity_sweep(vel0, state0)]
    for cycle in range(1, ITERS):
        stress_sweep(vel, state0 if cycle == 1 else state, state, fixed, rows, height)
        if cycle < ITERS - 1:
            sums.append(velocity_sweep(vel, state))

    tall = min(height, band)

    def last(base, diffs, acc):
        at = pl.ds(base, tall)
        new_u, new_v, gain = moved(vel, state, 0, base, tall, diffs, coriolis(base, tall))
        a, b, w = state[0, 0, at, :], state[1, 0, at, :], state[2, 0, at, :]
        row = base - PAD
        to = pl.ds(row, tall)
        vel_out[0, to, :] = new_u
        vel_out[1, to, :] = new_v
        sig_out[0, to, :] = 0.5 * (a + b)
        sig_out[1, to, :] = 0.5 * (a - b)
        sig_out[2, to, :] = 0.5 * w
        gap_e, gap_n = new_u - ocean[0, 0, at, :], new_v - ocean[1, 0, at, :]
        square = gap_e * gap_e + gap_n * gap_n + 0.01
        drag = square * lax.rsqrt(square) * fixed[1, 0, at, :]
        d = row // band
        within = row - d * band
        blocks[d, pl.ds(within, tall), :] = drag * gap_e
        blocks[d, pl.ds(band + within, tall), :] = drag * gap_n
        return acc + gain

    sums.append(sweep(state, (0, 2), PAD, rows // tall, tall, last, jnp.zeros((tall, cols), F32)))
    lines = [jnp.sum(s, axis=0, keepdims=True) for s in sums]
    tail = jnp.concatenate(lines + [jnp.zeros((DEPTH - ITERS, cols), F32)], axis=0)
    for k in range(n):
        blocks[k, 2 * band :, :] = tail


def unpack_out(n, got, out, sums):
    band, width = out.shape[1], out.shape[2]
    cols = width // n
    for k in range(n):
        for f in range(2):
            out[f, :, k * cols : (k + 1) * cols] = got[k, f * band : (f + 1) * band, :]
    total = got[0, 2 * band :, :]
    for k in range(1, n):
        total = total + got[k, 2 * band :, :]
    sums[...] = total


def total_sums(*refs):
    total = refs[0][...]
    for r in refs[1:-1]:
        total = total + r[...]
    refs[-1][...] = jnp.broadcast_to(jnp.sum(total, axis=1, keepdims=True), total.shape)


def local(velocity, stress, ice_mass, strength, land_mask, ocean_forcing):
    rows, cols = velocity.shape[1], velocity.shape[2]
    n, m = lax.axis_size("gx"), lax.axis_size("gy")
    band = ocean_forcing.shape[1]
    kinds = ocean_forcing.shape[0]
    xor = n & (n - 1) == 0 and n <= 8
    tall = rows + 2 * PAD
    me = lax.axis_index("gx")
    scal = jnp.stack([me, lax.axis_index("gy") * rows, m * rows]).astype(jnp.int32)

    def shift(x, axis, step):
        count = lax.axis_size(axis)
        return lax.ppermute(x, axis, [(i, (i + step) % count) for i in range(count)])

    def swap(x, axis, k):
        return lax.ppermute(x, axis, [(i, i ^ k) for i in range(lax.axis_size(axis))])

    fields = (velocity, stress, strength, ice_mass, land_mask)
    block = (kinds * band + SLOT, cols)
    slots = -(-n * SLOT // cols) * cols
    args = [pltpu.with_memory_space_constraint(x, pltpu.HBM) for x in fields + (ocean_forcing,)]
    own, to_right, to_left, *packed = call(
        functools.partial(pack, xor, n), "pack", 6,
        [(FIELDS, rows, cols)] + [(FIELDS * DEPTH, rows)] * 2 + ([block] * n if xor else [(n,) + block]),
        scratch=[
            pltpu.VMEM((rows, cols), jnp.int32), pltpu.VMEM(ocean_forcing.shape, F32), pltpu.VMEM((slots, cols), F32),
            pltpu.SemaphoreType.DMA((6,)),
        ],
        space=pl.BlockSpec(memory_space=pltpu.HBM),
    )(scal, *args)
    from_left = shift(to_right, "gx", 1)
    from_right = shift(to_left, "gx", -1)
    if xor:
        got = [packed[0]] + [None] * (n - 1)
        for k in range(n - 1, 0, -1):
            got[k] = swap(packed[k], "gx", k)
    else:
        got = [lax.all_to_all(packed[0], "gx", split_axis=0, concat_axis=0, tiled=True)]

    edge = (FIELDS, 2, DEPTH, cols)
    wings, to_up, to_down = call(extend_fields, "extend_fields", 3, [(FIELDS, rows, cols), edge, edge])(
        scal, own, from_left, from_right
    )
    bottom = shift(to_up, "gy", -1)
    top = shift(to_down, "gy", 1)

    def state_of(count):
        return (count, 2, tall, cols)

    vel0, state0, fixed = call(first_stress, "first_stress", 4, [state_of(2), state_of(3), state_of(3)])(
        scal, own, wings, top, bottom
    )
    edge = (kinds, 2, DEPTH, cols)
    forcing, f_up, f_down = call(
        functools.partial(extend_forcing, xor, n), "extend_forcing", len(got), [(kinds, 2, rows, cols), edge, edge],
        scratch=planes_of((slots, cols)),
    )(scal, *got)
    f_bottom = shift(f_up, "gy", -1)
    f_top = shift(f_down, "gy", 1)
    vel, sig, blocks = call(
        functools.partial(subcycles, n), "subcycles", 6, [velocity.shape, stress.shape, (n, 2 * band + DEPTH, cols)],
        scratch=planes_of(state_of(2), state_of(3), state_of(2), state_of(2)),
    )(scal, vel0, state0, fixed, forcing, f_top, f_bottom)
    back = lax.all_to_all(blocks, "gx", split_axis=0, concat_axis=0, tiled=True)
    ocean_stress, sums = call(
        functools.partial(unpack_out, n), "unpack_out", 1, [(2, band, n * cols), (DEPTH, cols)], scalars=0
    )(back)
    others = [sums] + [shift(sums, "gy", k) for k in range(1, m)]
    (history,) = call(total_sums, "total_sums", m, [(DEPTH, cols)], scalars=0)(*others)
    return vel, sig, history[:ITERS, 0], ocean_stress


def solution(mesh):
    placed = (
        P(None, "gy", "gx"),
        P(None, "gy", "gx"),
        P("gy", "gx"),
        P("gy", "gx"),
        P("gy", "gx"),
        P(None, ("gy", "gx"), None),
    )
    return jax.shard_map(
        local,
        mesh=mesh,
        in_specs=placed,
        out_specs=(P(None, "gy", "gx"), P(None, "gy", "gx"), P(), P(None, ("gy", "gx"), None)),
        check_vma=False,
    )
```

```python
import functools

import jax
import jax.numpy as jnp
from jax import lax
from jax.experimental import pallas as pl
from jax.experimental.pallas import tpu as pltpu
from jax.sharding import PartitionSpec as P


ITERS = 4
DELTA_FLOOR = 0.0025
DEPTH = 2 * ITERS
SLOT = 2 * DEPTH
FIELDS = 8
PAD = 2 * DEPTH

SMEM = pl.BlockSpec(memory_space=pltpu.SMEM)
VMEM = pl.BlockSpec(memory_space=pltpu.VMEM)
HBM = pl.BlockSpec(memory_space=pltpu.HBM)
F32 = jnp.float32
VMEM_LIMIT = 16 * 1024 * 1024


def call(body, n_in, outs, scratch=(), space=VMEM, out_space=VMEM):
    return pl.pallas_call(
        body,
        out_shape=[jax.ShapeDtypeStruct(s, F32) for s in outs],
        in_specs=[space] * n_in,
        out_specs=[out_space] * len(outs),
        scratch_shapes=scratch,
        compiler_params=pltpu.CompilerParams(vmem_limit_bytes=VMEM_LIMIT),
    )


def planes_of(*shapes):
    return [pltpu.VMEM(s, F32) for s in shapes]


def lane_of(shape):
    return lax.broadcasted_iota(jnp.int32, shape, 1)


def slot_start(index):
    return SLOT * index


def transposed(tile, lanes):
    rows = tile.shape[0]
    if rows < lanes:
        tile = jnp.concatenate([tile, jnp.zeros((lanes - rows, lanes), F32)], axis=0)
    parts = [tile[i : i + lanes].T for i in range(0, tile.shape[0], lanes)]
    return parts[0] if len(parts) == 1 else jnp.concatenate(parts, axis=1)


def fetch(pairs, sems):
    copies = [pltpu.make_async_copy(src, dst, sems.at[i]) for i, (src, dst) in enumerate(pairs)]
    for c in copies:
        c.start()
    for c in copies:
        c.wait()


def pack_fields(vel, sig, strength, mass, mask, own, to_right, to_left, mask_ref, sems):
    pairs = ((vel, own.at[0:2]), (sig, own.at[2:5]), (strength, own.at[5]), (mass, own.at[6]), (mask, mask_ref))
    fetch(pairs, sems)
    own[7] = mask_ref[...].astype(F32)
    cols = own.shape[2]
    lane = lane_of(own.shape[1:])
    tile = jnp.zeros(own.shape[1:], F32)
    for i in range(FIELDS):
        start = slot_start(i)
        moved = pltpu.roll(own[i], (DEPTH + start) % cols, 1)
        tile = jnp.where((lane >= start) & (lane < start + SLOT), moved, tile)
    turned = transposed(tile, cols)
    for i in range(FIELDS):
        start = slot_start(i)
        to_right[i * DEPTH : (i + 1) * DEPTH, :] = turned[start : start + DEPTH]
        to_left[i * DEPTH : (i + 1) * DEPTH, :] = turned[start + DEPTH : start + SLOT]


def pack_forcing(xor, n, band_hbm, *refs):
    outs, (band, turned_ref, sems) = refs[:-3], refs[-3:]
    fetch(((band_hbm, band),), sems)
    kinds, rows, width = band.shape
    cols = width // n
    height = kinds * rows
    me = lax.axis_index("gx")
    lane = lane_of((height, cols))
    per_tile = cols // SLOT
    tiles = [band[:, :, d * cols : (d + 1) * cols].reshape(height, cols) for d in range(n)]
    for first in range(0, n, per_tile):
        packed = jnp.zeros((height, cols), F32)
        for d in range(first, min(first + per_tile, n)):
            start = slot_start(d - first)
            halo = jnp.where(lane < cols // 2, tiles[(d + 1) % n], tiles[(d - 1) % n])
            moved = pltpu.roll(halo, (DEPTH + start) % cols, 1)
            packed = jnp.where((lane >= start) & (lane < start + SLOT), moved, packed)
        turned_ref[first * SLOT : first * SLOT + cols, :] = transposed(packed, cols)
    for k in range(n):
        d = me ^ k if xor else k
        out = outs[k] if xor else outs[0].at[k]
        at = pl.multiple_of(d * cols, cols) if xor else d * cols
        out[:height, :] = band[:, :, pl.ds(at, cols)].reshape(height, cols)
        at = pl.multiple_of(d * SLOT, SLOT) if xor else d * SLOT
        out[height:, :] = turned_ref[pl.ds(at, SLOT), :]


def extend_fields(own, from_left, from_right, wings, to_up, to_down):
    _, rows, cols = own.shape
    pieces = []
    for i in range(FIELDS):
        pieces.append(from_left[i * DEPTH : (i + 1) * DEPTH, :])
        pieces.append(from_right[i * DEPTH : (i + 1) * DEPTH, :])
    turned = jnp.concatenate(pieces, axis=0)
    halo = jnp.concatenate([turned[:, i : i + cols].T for i in range(0, rows, cols)], axis=0)
    for i in range(FIELDS):
        wing = pltpu.roll(halo, (-(DEPTH + slot_start(i))) % cols, 1)
        wings[i] = wing
        to_up[i, 0] = own[i, :DEPTH, :]
        to_up[i, 1] = wing[:DEPTH]
        to_down[i, 0] = own[i, rows - DEPTH :, :]
        to_down[i, 1] = wing[rows - DEPTH :]


def shifted(ref, base, height, step):
    return ref.at[pl.ds(base - DEPTH, height + 2 * DEPTH), :][DEPTH + step : DEPTH + step + height, :]


def down_up(ref, at, base, height):
    return shifted(ref.at[at], base, height, 1) - shifted(ref.at[at], base, height, -1)


def east_west(main, wing):
    cols = main.shape[1]
    lane = lane_of(main.shape)
    east_m, east_w = pltpu.roll(main, cols - 1, 1), pltpu.roll(wing, cols - 1, 1)
    west_m, west_w = pltpu.roll(main, 1, 1), pltpu.roll(wing, 1, 1)
    end, begin = lane == cols - 1, lane == 0
    return (
        jnp.where(end, east_w, east_m) - jnp.where(begin, west_w, west_m),
        jnp.where(end, east_m, east_w) - jnp.where(begin, west_m, west_w),
    )


def east_west_of(ref, plane, base, height):
    at = pl.ds(base, height)
    return east_west(ref[plane, 0, at, :], ref[plane, 1, at, :])


def row_blocks(rows, height):
    own = [(PAD + r, height) for r in range(0, rows, height)]
    return [(DEPTH, DEPTH)] + own + [(PAD + rows, DEPTH)]


def sweep(ref, planes, blocks, body):
    for base, height in blocks:
        body(base, height, [east_west_of(ref, p, base, height) for p in planes])


def stress_sweep(vel, old, new, fixed, rows):
    def body(base, height, diffs):
        at = pl.ds(base, height)
        for s in range(2):
            ux, vx = diffs[0][s], diffs[1][s]
            uy = down_up(vel, (0, s), base, height)
            vy = down_up(vel, (1, s), base, height)
            p4, ice = fixed[0, s, at, :], fixed[1, s, at, :]
            div = 0.5 * (ux + vy)
            ten = 0.125 * (ux - vy)
            shear = 0.125 * (uy + vx)
            inv = lax.rsqrt(div * div + 4.0 * (ten * ten + shear * shear) + DELTA_FLOOR)
            pr = p4 * inv
            keep = 0.75 * ice
            new[0, s, at, :] = keep * old[0, s, at, :] + (pr * (div + ten) - p4)
            new[1, s, at, :] = keep * old[1, s, at, :] + (pr * (div - ten) - p4)
            new[2, s, at, :] = keep * old[2, s, at, :] + pr * shear

    sweep(vel, (0, 1), row_blocks(rows, 2 * DEPTH), body)


def first_stress(own, wings, top, bottom, vel, state, fixed):
    rows = own.shape[1]
    band, bands = lax.axis_index("gy"), lax.axis_size("gy")
    height = 2 * DEPTH

    def setup(base, count, s, get, alive):
        at = pl.ds(base, count)
        keep = (lambda x: x) if alive is None else (lambda x: jnp.where(alive, x, 0.0))
        ice = keep(get(7))
        vel[0, s, at, :] = keep(get(0))
        vel[1, s, at, :] = keep(get(1))
        s0, s1 = get(2), get(3)
        state[0, s, at, :] = s0 + s1
        state[1, s, at, :] = s0 - s1
        state[2, s, at, :] = 2.0 * get(4)
        fixed[0, s, at, :] = 0.25 * get(5) * ice
        fixed[1, s, at, :] = ice
        fixed[2, s, at, :] = 1.0 / get(6)

    for s in range(2):
        setup(DEPTH, DEPTH, s, lambda i: top[i, s], band > 0)
        setup(PAD + rows, DEPTH, s, lambda i: bottom[i, s], band < bands - 1)

    for base in range(0, rows, height):
        for s, src in enumerate((own, wings)):
            setup(PAD + base, height, s, lambda i: src[i, pl.ds(base, height), :], None)
    stress_sweep(vel, state, state, fixed, rows)


def unturned(piece, cols):
    if piece.shape[0] < cols:
        piece = jnp.concatenate([piece, jnp.zeros((cols - piece.shape[0], cols), F32)], axis=0)
    return piece.T


def edge_forcing(xor, n, *refs):
    blocks, (to_up, to_down) = refs[:-2], refs[-2:]
    kinds, _, _, cols = to_up.shape
    me = lax.axis_index("gx")
    height = (blocks[0].shape[0] if xor else blocks[0].shape[1]) - SLOT
    band = height // kinds

    def send(block, out, begin):
        wing = pltpu.roll(unturned(block[height : height + SLOT, :], cols), (-DEPTH) % cols, 1)
        for f in range(kinds):
            lo = f * band + begin
            out[f, 0] = block[lo : lo + DEPTH, :]
            out[f, 1] = wing[lo : lo + DEPTH]

    for k in range(n if xor else 0):
        pl.when(me == k)(functools.partial(send, blocks[k], to_up, 0))
        pl.when(me == k ^ (n - 1))(functools.partial(send, blocks[k], to_down, band - DEPTH))
    if not xor:
        send(blocks[0].at[0], to_up, 0)
        send(blocks[0].at[n - 1], to_down, band - DEPTH)


def extend_forcing(xor, n, vel, fixed, *refs):
    blocks, (start, ocean, turned_ref) = refs[:-3], refs[-3:]
    me = lax.axis_index("gx")
    _, _, rows, cols = ocean.shape
    band = rows // n
    height = 4 * band
    per_tile = cols // SLOT

    def put(base, s, get):
        to, at = pl.ds(base, band), pl.ds(PAD + base, band)
        im = fixed[2, s, at, :]
        start[0, s, to, :] = vel[0, s, at, :] + get(0) * im
        start[1, s, to, :] = vel[1, s, at, :] + get(1) * im
        ocean[0, s, to, :] = get(2)
        ocean[1, s, to, :] = get(3)

    def base_of(k):
        return pl.multiple_of((me ^ k) * band, DEPTH) if xor else k * band

    for k in range(n):
        block = blocks[k] if xor else blocks[0].at[k]
        put(base_of(k), 0, lambda f: block[f * band : (f + 1) * band, :])
        turned_ref[k * SLOT : (k + 1) * SLOT, :] = block[height : height + SLOT, :]
    for first in range(0, n, per_tile):
        last = min(first + per_tile, n)
        halo = unturned(turned_ref[first * SLOT : last * SLOT, :], cols)
        for k in range(first, last):
            wing = pltpu.roll(halo, (-(DEPTH + slot_start(k - first))) % cols, 1)
            put(base_of(k), 1, lambda f: wing[f * band : (f + 1) * band])


def subcycles(n, vel0, state0, fixed, start, ocean, top, bottom, vel_out, sig_out, blocks, vel, state, start_ref, ocean_ref):
    rows, cols = vel_out.shape[1:]
    height = 2 * DEPTH
    band = rows // n
    row_start = lax.axis_index("gy") * rows
    slope = 1.2 / (lax.axis_size("gy") * rows)

    def coriolis(base, tall):
        row = lax.broadcasted_iota(jnp.int32, (tall, cols), 0) + (row_start + (base - PAD))
        return 0.3 + slope * (row.astype(F32) + 0.5)

    for e, (base, edge) in enumerate(((DEPTH, top), (PAD + rows, bottom))):
        at = pl.ds(base, DEPTH)
        for s in range(2):
            for i in range(2):
                start_ref[e, i, s] = vel0[i, s, at, :] + edge[i, s] * fixed[2, s, at, :]
                ocean_ref[e, i, s] = edge[2 + i, s]

    def held(own, edges, i, s, base, tall):
        if base < PAD:
            return edges[0, i, s]
        if base >= PAD + rows:
            return edges[1, i, s]
        return own[i, s, base - PAD : base - PAD + tall, :]

    def moved(old, now, s, base, tall, diffs, cor):
        at = pl.ds(base, tall)
        ge = diffs[0][s] + down_up(now, (2, s), base, tall)
        gn = diffs[1][s] + down_up(now, (1, s), base, tall)
        u, v = old[0, s, at, :], old[1, s, at, :]
        oe, on = (held(ocean, ocean_ref, i, s, base, tall) for i in range(2))
        be, bn = (held(start, start_ref, i, s, base, tall) for i in range(2))
        im, ice = fixed[2, s, at, :], fixed[1, s, at, :]
        gap_e, gap_n = oe - u, on - v
        square = gap_e * gap_e + gap_n * gap_n + 0.01
        pull = square * lax.rsqrt(square) * im
        inv = ice / (pull + 5.0)
        im4 = 0.25 * im
        new_u = (4.0 * u + be + ge * im4 + pull * oe + cor * v) * inv
        new_v = (4.0 * v + bn + gn * im4 + pull * on - cor * u) * inv
        du, dv = new_u - u, new_v - v
        return new_u, new_v, du * du + dv * dv

    def line(acc, gain):
        return acc + jnp.sum(gain.reshape(gain.shape[0] // DEPTH, DEPTH, cols), axis=0)

    def velocity_sweep(old, now):
        acc = [jnp.zeros((DEPTH, cols), F32)]

        def body(base, tall, diffs):
            at = pl.ds(base, tall)
            cor = coriolis(base, tall)
            for s in range(2):
                new_u, new_v, gain = moved(old, now, s, base, tall, diffs, cor)
                vel[0, s, at, :] = new_u
                vel[1, s, at, :] = new_v
                if s == 0 and PAD <= base < PAD + rows:
                    acc[0] = line(acc[0], gain)

        sweep(now, (0, 2), row_blocks(rows, height), body)
        return acc[0]

    sums = [velocity_sweep(vel0, state0)]
    for cycle in range(1, ITERS):
        stress_sweep(vel, state0 if cycle == 1 else state, state, fixed, rows)
        if cycle < ITERS - 1:
            sums.append(velocity_sweep(vel, state))

    tall = min(height, band)
    acc = [jnp.zeros((DEPTH, cols), F32)]

    def last(base, tall, diffs):
        at = pl.ds(base, tall)
        new_u, new_v, gain = moved(vel, state, 0, base, tall, diffs, coriolis(base, tall))
        a, b, w = state[0, 0, at, :], state[1, 0, at, :], state[2, 0, at, :]
        row = base - PAD
        to = pl.ds(row, tall)
        vel_out[0, to, :] = new_u
        vel_out[1, to, :] = new_v
        sig_out[0, to, :] = 0.5 * (a + b)
        sig_out[1, to, :] = 0.5 * (a - b)
        sig_out[2, to, :] = 0.5 * w
        gap_e, gap_n = new_u - ocean[0, 0, to, :], new_v - ocean[1, 0, to, :]
        square = gap_e * gap_e + gap_n * gap_n + 0.01
        drag = square * lax.rsqrt(square) * fixed[1, 0, at, :]
        d = row // band
        within = row - d * band
        blocks[d, pl.ds(within, tall), :] = drag * gap_e
        blocks[d, pl.ds(band + within, tall), :] = drag * gap_n
        acc[0] = line(acc[0], gain)

    sweep(state, (0, 2), [(PAD + r, tall) for r in range(0, rows, tall)], last)
    sums.append(acc[0])
    lines = [jnp.sum(s, axis=0, keepdims=True) for s in sums]
    tail = jnp.concatenate(lines + [jnp.zeros((DEPTH - ITERS, cols), F32)], axis=0)
    for k in range(n):
        blocks[k, 2 * band :, :] = tail


def emit(vel, sig, vel_out, sig_out, sems):
    fetch(((vel, vel_out), (sig, sig_out)), sems)


def sum_lines(n, got, sums):
    at = slice(got.shape[1] - DEPTH, None)
    total = got[0, at, :]
    for k in range(1, n):
        total = total + got[k, at, :]
    sums[...] = total


def unpack_out(n, got, out):
    band, width = out.shape[1], out.shape[2]
    cols = width // n
    for k in range(n):
        for f in range(2):
            out[f, :, k * cols : (k + 1) * cols] = got[k, f * band : (f + 1) * band, :]


def total_sums(*refs):
    total = refs[0][...]
    for r in refs[1:-1]:
        total = total + r[...]
    for k in range(ITERS):
        refs[-1][k] = jnp.sum(total[k : k + 1, :])


def shift(x, axis, step):
    count = lax.axis_size(axis)
    return lax.ppermute(x, axis, [(i, (i + step) % count) for i in range(count)])


def swap(x, axis, k):
    return lax.ppermute(x, axis, [(i, i ^ k) for i in range(lax.axis_size(axis))])


def local(velocity, stress, ice_mass, strength, land_mask, ocean_forcing):
    rows, cols = velocity.shape[1], velocity.shape[2]
    n, m = lax.axis_size("gx"), lax.axis_size("gy")
    band = ocean_forcing.shape[1]
    kinds = ocean_forcing.shape[0]
    xor = direct(n)
    tall = rows + 2 * PAD

    def state_of(count):
        return (count, 2, tall, cols)

    def in_hbm(x):
        return pltpu.with_memory_space_constraint(x, pltpu.HBM)

    block = (kinds * band + SLOT, cols)
    slots = -(-n * SLOT // cols) * cols
    packed = call(
        functools.partial(pack_forcing, xor, n), 1, [block] * n if xor else [(n,) + block],
        scratch=planes_of(ocean_forcing.shape, (slots, cols)) + [pltpu.SemaphoreType.DMA((1,))], space=HBM,
    )(in_hbm(ocean_forcing))
    if xor:
        got = [packed[0]] + [None] * (n - 1)
        for k in range(n - 1, 0, -1):
            got[k] = swap(packed[k], "gx", k)
    else:
        got = [lax.all_to_all(packed[0], "gx", split_axis=0, concat_axis=0, tiled=True)]

    fields = (velocity, stress, strength, ice_mass, land_mask)
    own, to_right, to_left = call(
        pack_fields, 5, [(FIELDS, rows, cols)] + [(FIELDS * DEPTH, rows)] * 2,
        scratch=[pltpu.VMEM((rows, cols), jnp.int32), pltpu.SemaphoreType.DMA((5,))], space=HBM,
    )(*map(in_hbm, fields))
    from_left = shift(to_right, "gx", 1)
    from_right = shift(to_left, "gx", -1)
    edge = (FIELDS, 2, DEPTH, cols)
    wings, to_up, to_down = call(extend_fields, 3, [(FIELDS, rows, cols), edge, edge])(own, from_left, from_right)
    bottom = shift(to_up, "gy", -1)
    top = shift(to_down, "gy", 1)
    vel0, state0, fixed = call(first_stress, 4, [state_of(2), state_of(3), state_of(3)])(own, wings, top, bottom)

    edge = (kinds, 2, DEPTH, cols)
    f_up, f_down = call(functools.partial(edge_forcing, xor, n), len(got), [edge, edge])(*got)
    f_bottom = shift(f_up, "gy", -1)
    f_top = shift(f_down, "gy", 1)
    start, ocean = call(
        functools.partial(extend_forcing, xor, n), 2 + len(got), [(2, 2, rows, cols)] * 2,
        scratch=planes_of((slots, cols)),
    )(vel0, fixed, *got)
    vel, sig, blocks = call(
        functools.partial(subcycles, n), 7, [velocity.shape, stress.shape, (n, 2 * band + DEPTH, cols)],
        scratch=planes_of(state_of(2), state_of(3), (2, 2, 2, DEPTH, cols), (2, 2, 2, DEPTH, cols)),
    )(vel0, state0, fixed, start, ocean, f_top, f_bottom)

    back = lax.all_to_all(blocks, "gx", split_axis=0, concat_axis=0, tiled=True)
    vel, sig = call(
        emit, 2, [velocity.shape, stress.shape], scratch=[pltpu.SemaphoreType.DMA((2,))], out_space=HBM
    )(vel, sig)
    (sums,) = call(functools.partial(sum_lines, n), 1, [(DEPTH, cols)])(back)
    others = [sums] + [shift(sums, "gy", k) for k in range(1, m)]
    (ocean_stress,) = call(functools.partial(unpack_out, n), 1, [(2, band, n * cols)])(back)
    (history,) = call(total_sums, m, [(ITERS,)], out_space=SMEM)(*others)
    return vel, sig, history, ocean_stress


def direct(n):
    return n & (n - 1) == 0 and n <= 8


def solution(mesh):
    placed = (
        P(None, "gy", "gx"),
        P(None, "gy", "gx"),
        P("gy", "gx"),
        P("gy", "gx"),
        P("gy", "gx"),
        P(None, ("gy", "gx"), None),
    )
    return jax.shard_map(
        local,
        mesh=mesh,
        in_specs=placed,
        out_specs=(P(None, "gy", "gx"), P(None, "gy", "gx"), P(), P(None, ("gy", "gx"), None)),
        check_vma=False,
    )
```
